32 devices in a mesh: rep: 2 (over x), dp: 16 (over y, z, core).
Axes of the slice: x: 2, y: 2, z: 4, core: 2. Of those that a mesh axis runs over, the one named last changes fastest.
Arguments:
- x: bfloat16 [32, 2048, 1024], P(('rep', 'dp')), parts along dimension 0
- dy: bfloat16 [32, 2048, 1024], P(('rep', 'dp')), parts along dimension 0
- w_gate: bfloat16 [2, 1024, 4096], replicated
- w_up: bfloat16 [2, 1024, 4096], replicated
- w_down: bfloat16 [2, 4096, 1024], replicated
- m_w_gate: float32 [2, 1024, 4096], replicated
- m_w_up: float32 [2, 1024, 4096], replicated
- m_w_down: float32 [2, 4096, 1024], replicated
- v_w_gate: float32 [2, 1024, 4096], replicated
- v_w_up: float32 [2, 1024, 4096], replicated
- v_w_down: float32 [2, 4096, 1024], replicated
Outputs:
- output 1: bfloat16 [4, 1024, 4096], P('rep'), parts along dimension 0
- output 2: bfloat16 [4, 1024, 4096], P('rep'), parts along dimension 0
- output 3: bfloat16 [4, 4096, 1024], P('rep'), parts along dimension 0
- output 4: float32 [4, 1024, 4096], P('rep'), parts along dimension 0
- output 5: float32 [4, 1024, 4096], P('rep'), parts along dimension 0
- output 6: float32 [4, 4096, 1024], P('rep'), parts along dimension 0
- output 7: float32 [4, 1024, 4096], P('rep'), parts along dimension 0
- output 8: float32 [4, 1024, 4096], P('rep'), parts along dimension 0
- output 9: float32 [4, 4096, 1024], P('rep'), parts along dimension 0
There are 2 independent parts. The reference program is written for one: setup_inputs(seed, part) draws one part's arguments, and reference() takes and returns one part's arrays. A program takes and returns all parts, laid end to end along the dimension named above; an argument that names none is the same for every part.
All inputs are finite; a program needn't handle non-finite values.
Results may differ from the reference program's by a relative error of at most 0.022.
Values are sent between devices in bfloat16 or wider.
A program may use at most 2.75 GiB of HBM per device.

```python
import jax
import jax.numpy as jnp
from jax import lax

SEQUENCES = 16
TOKENS = 2048
D = 1024
FF = 4096
LAYERS = 2
NAMES = ("w_gate", "w_up", "w_down")
SHAPES = {"w_gate": (LAYERS, D, FF), "w_up": (LAYERS, D, FF), "w_down": (LAYERS, FF, D)}


def bump(key, n, height):
    away = (jnp.arange(n, dtype=jnp.int32) - jax.random.randint(key, (), 0, n, jnp.int32)) % n
    return jnp.where(away < n // 8, height, 1.0)


def together(key, own, strength):
    shared = jax.random.normal(key, own.shape[1:], jnp.float32)
    return (own + strength * shared) * lax.rsqrt(1 + strength * strength)


def setup_inputs(seed: int = 0, part: int = 0) -> dict:
    kx, kdy, ka, kb, kz, kf, kh, kl, *keys = jax.random.split(jax.random.key(seed), 8 + 3 * len(NAMES))
    kx, kdy, ka, kb = (jax.random.fold_in(k, part) for k in (kx, kdy, ka, kb))
    kw, km, kv = (keys[i::3] for i in range(3))
    shape = (SEQUENCES, TOKENS, D)
    much_x, much_dy = jax.random.uniform(kz, (2,), jnp.float32, 0.0, 1.0)
    loud = 2.0 ** jax.random.uniform(jax.random.fold_in(kz, 1), (), jnp.float32, -1.0, 2.0)
    layers = 2.0 ** jax.random.uniform(kl, (LAYERS, 1, 1), jnp.float32, -1.0, 1.0)
    x = together(ka, jax.random.normal(kx, shape, jnp.float32), much_x) * bump(kf, D, 4.0)
    dy = together(kb, jax.random.normal(kdy, shape, jnp.float32), much_dy)
    drawn = {"x": x.astype(jnp.bfloat16), "dy": (loud * dy * (SEQUENCES * TOKENS) ** -0.5).astype(jnp.bfloat16)}
    for key, name in zip(kw, NAMES, strict=True):
        w = jax.random.normal(key, SHAPES[name], jnp.float32) * SHAPES[name][1] ** -0.5
        drawn[name] = (w * {"w_gate": 1.0, "w_up": bump(kh, FF, 4.0), "w_down": layers}[name]).astype(jnp.bfloat16)
    for key, name in zip(km, NAMES, strict=True):
        drawn[f"m_{name}"] = 0.1 * jax.random.normal(key, SHAPES[name], jnp.float32)
    for key, name in zip(kv, NAMES, strict=True):
        drawn[f"v_{name}"] = jax.random.uniform(key, SHAPES[name], jnp.float32, 0.005, 0.015)
    return drawn


def matmul(a, w):
    return jnp.dot(a, w, preferred_element_type=jnp.float32).astype(jnp.bfloat16)


def normed(h):
    wide = h.astype(jnp.float32)
    scale = lax.rsqrt(jnp.mean(wide**2, -1, keepdims=True) + 1e-6)
    return (wide * scale).astype(jnp.bfloat16)


def layer(h, w):
    a = normed(h)
    gate = jnp.dot(a, w["w_gate"], preferred_element_type=jnp.float32)
    up = jnp.dot(a, w["w_up"], preferred_element_type=jnp.float32)
    return h + matmul((jax.nn.silu(gate) * up).astype(jnp.bfloat16), w["w_down"])


def adamw(w, m, v, g):
    m = 0.9 * m + 0.1 * g
    v = 0.95 * v + 0.05 * g * g
    step = m * lax.rsqrt(v + 1e-8) + 0.1 * w
    return (w - 0.02 * step).astype(jnp.bfloat16), m, v


def stack(weights, h):
    return lax.scan(lambda h, w: (layer(h, w), None), h, weights)[0]


def reference(x, dy, w_gate, w_up, w_down, m_w_gate, m_w_up, m_w_down, v_w_gate, v_w_up, v_w_down):
    weights = dict(zip(NAMES, (w_gate, w_up, w_down), strict=True))

    def take(so_far, sequence):
        h, by_y = sequence
        _, back = jax.vjp(lambda w: stack(w, h), weights)
        return jax.tree.map(lambda total, term: total + term.astype(jnp.float32), so_far, back(by_y)[0]), None

    none_yet = {name: jnp.zeros(w.shape, jnp.float32) for name, w in weights.items()}
    by_weights, _ = lax.scan(take, none_yet, (x, dy))
    gradients = [by_weights[name].astype(jnp.bfloat16).astype(jnp.float32) for name in NAMES]
    new = [
        adamw(w.astype(jnp.float32), m, v, g)
        for w, m, v, g in zip((w_gate, w_up, w_down), (m_w_gate, m_w_up, m_w_down), (v_w_gate, v_w_up, v_w_down), gradients, strict=True)
    ]
    return tuple(one[which] for which in range(3) for one in new)
```

```python
import jax
import jax.numpy as jnp
from jax import lax
from jax.experimental import pallas as pl
from jax.experimental.pallas import tpu as pltpu
from jax.sharding import PartitionSpec as P


CHIPS = 8


def dot(a, b, over):
    return lax.dot_general(a, b, (((over[0],), (over[1],)), ((), ())), preferred_element_type=jnp.float32)


def normed(h):
    wide = h.astype(jnp.float32)
    scale = lax.rsqrt(jnp.mean(wide**2, -1, keepdims=True) + 1e-6)
    return (wide * scale).astype(jnp.bfloat16)


def device_at(place, core):
    place = place if core == 0 else CHIPS - 1 - place
    y, z = (0, place) if place < CHIPS // 2 else (1, CHIPS - 1 - place)
    return (y * (CHIPS // 2) + z) * 2 + core


NEXT = [(device_at(q, core), device_at((q + 1) % CHIPS, core)) for core in range(2) for q in range(CHIPS)]
BACK = [(to, of) for of, to in NEXT]
SWAP = [(d, d ^ 1) for d in range(2 * CHIPS)]


def where_am_i():
    index = lax.axis_index("dp")
    core = index % 2
    chip = index // 2
    z, y = chip % (CHIPS // 2), chip // (CHIPS // 2)
    place = jnp.where(y == 0, z, CHIPS - 1 - z)
    return core, jnp.where(core == 0, place, CHIPS - 1 - place)


def take(array, index):
    return lax.dynamic_index_in_dim(array, index, 0, keepdims=False)


def permuted(array, pairs):
    return lax.ppermute(array, "dp", pairs)


PARTS = ((0, -1, 1, -2, 2), (-3, 3, -4))


def summed_over_group(g, core, q):
    rows, columns = g.shape
    g = g.reshape(2, CHIPS, rows // (2 * CHIPS), columns)
    own = take(g, core)
    other = permuted(take(g, 1 - core), SWAP)

    def local(ahead):
        chunk = (q + CHIPS + ahead) % CHIPS
        return take(own, chunk).astype(jnp.float32) + take(other, chunk).astype(jnp.float32)

    half = CHIPS // 2
    right, left = local(half), None
    for stage in range(1, half + 1):
        right = permuted(right.astype(jnp.bfloat16), NEXT).astype(jnp.float32)
        if stage == 1:
            left = local(1 - half)
        else:
            left = permuted(left.astype(jnp.bfloat16), BACK).astype(jnp.float32)
        if stage < half:
            right = right + local(half - stage)
            if stage > 1:
                left = left + local(stage - half)
    final = (right + left + local(0)).astype(jnp.bfloat16)
    behind, ahead = [final], [final]
    for stage in range(1, half + 1):
        behind.append(permuted(behind[-1], NEXT))
        if stage < half:
            ahead.append(permuted(ahead[-1], BACK))
    for order in PARTS:
        mine = jnp.stack([behind[-n] if n <= 0 else ahead[n] for n in order])
        yield order, mine, permuted(mine, SWAP)


def adamw_kernel(at, order, w, m, v, mine, theirs, *rest):
    new_w, new_m, new_v = rest[-3:]
    g = jnp.where(pl.program_id(0) == 0, mine[0].astype(jnp.float32), theirs[0].astype(jnp.float32))
    m = 0.9 * m[0] + 0.1 * g
    v = 0.95 * v[0] + 0.05 * g * g
    wide = w[0].astype(jnp.float32)
    step = m * lax.rsqrt(v + 1e-8) + 0.1 * wide
    new_w[0] = (wide - 0.02 * step).astype(jnp.bfloat16)
    new_m[0] = m
    new_v[0] = v


def adamw(number, w, m, v, mine, theirs, at, order, so_far):
    _, rows, columns = w.shape
    block = rows // (2 * CHIPS)
    chunks = len(order)
    order = jnp.array(order, jnp.int32)

    def place(t, s, at, order):
        half = jnp.where(t == 0, at[0], 1 - at[0])
        q = jnp.where(t == 0, at[1], CHIPS - 1 - at[1])
        return number, half * CHIPS + lax.rem(q + CHIPS + order[s], CHIPS), 0

    spec = pl.BlockSpec((1, block, columns), place)
    in_specs = [
        spec,
        spec,
        spec,
        pl.BlockSpec((1, block, columns), lambda t, s, at, order: (jnp.where(t == 0, s, chunks - 1), 0, 0)),
        pl.BlockSpec((1, block, columns), lambda t, s, at, order: (jnp.where(t == 0, 0, s), 0, 0)),
    ] + [pl.BlockSpec(memory_space=pl.ANY)] * len(so_far)
    return pl.pallas_call(
        adamw_kernel,
        grid_spec=pltpu.PrefetchScalarGridSpec(
            num_scalar_prefetch=2, grid=(2, chunks), in_specs=in_specs, out_specs=[spec] * 3
        ),
        out_shape=[jax.ShapeDtypeStruct(w.shape, dtype) for dtype in (jnp.bfloat16, jnp.float32, jnp.float32)],
        input_output_aliases={7 + i: i for i in range(len(so_far))},
        compiler_params=pltpu.CompilerParams(
            dimension_semantics=("arbitrary", "arbitrary"), vmem_limit_bytes=32 * 2**20
        ),
        cost_estimate=pl.CostEstimate(
            flops=40 * chunks * block * columns,
            bytes_accessed=44 * chunks * block * columns,
            transcendentals=2 * chunks * block * columns,
        ),
    )(at, order, w, m, v, mine, theirs, *so_far)


def solution(mesh):
    def whole(x, dy, *arrays):
        weights, m, v = (arrays[i : i + 3] for i in (0, 3, 6))
        layers = weights[0].shape[0]
        core, q = where_am_i()
        at = jnp.stack([core, q]).astype(jnp.int32)
        h, kept = x[0], []
        for number in range(layers):
            w_gate, w_up, w_down = (w[number] for w in weights)
            a, back = jax.vjp(normed, h)
            gate, up = dot(a, w_gate, (1, 0)), dot(a, w_up, (1, 0))
            act = (jax.nn.silu(gate) * up).astype(jnp.bfloat16)
            gate, up, act = lax.optimization_barrier((gate, up, act))
            kept.append((a, gate, up, act, back))
            if number < layers - 1:
                h = h + dot(act, w_down, (1, 0)).astype(jnp.bfloat16)
        by_h, new = dy[0], [()] * 3
        for number in reversed(range(layers)):
            w_gate, w_up, w_down = (w[number] for w in weights)
            a, gate, up, act, back = kept[number]

            def take_step(i, g):
                for order, mine, theirs in summed_over_group(g, core, q):
                    new[i] = adamw(number, weights[i], m[i], v[i], mine, theirs, at, order, new[i])

            g = dot(act, by_h, (0, 0)).astype(jnp.bfloat16)
            take_step(2, g)
            by_act = dot(by_h, w_down, (1, 1)).astype(jnp.bfloat16).astype(jnp.float32)
            gated, back_silu = jax.vjp(jax.nn.silu, gate)
            by_up = (by_act * gated).astype(jnp.bfloat16)
            by_gate = back_silu(by_act * up)[0].astype(jnp.bfloat16)
            by_gate, by_up = lax.optimization_barrier((by_gate, by_up))
            g = dot(a, by_gate, (0, 0)).astype(jnp.bfloat16)
            take_step(0, g)
            g = dot(a, by_up, (0, 0)).astype(jnp.bfloat16)
            take_step(1, g)
            if number:
                by_a = dot(by_gate, w_gate, (1, 1)).astype(jnp.bfloat16)
                by_a = lax.optimization_barrier(by_a)
                by_a = by_a + dot(by_up, w_up, (1, 1)).astype(jnp.bfloat16)
                by_a = lax.optimization_barrier(by_a)
                by_h = by_h + back(by_a)[0]
        return tuple(one[which] for which in range(3) for one in new)

    return jax.shard_map(
        whole,
        mesh=mesh,
        in_specs=(P(("rep", "dp"), None, None),) * 2 + (P(None, None, None),) * 9,
        out_specs=(P("rep", None, None),) * 9,
        check_vma=False,
    )
```
